32 devices in a mesh: ens: 2 (over y), box: 4 (over z), slab: 4 (over x, core).
Axes of the slice: x: 2, y: 2, z: 4, core: 2. Of those that a mesh axis runs over, the one named last changes fastest.
Arguments:
- pressure_now: float32 [4, 64, 64, 256], P('ens', 'box', 'slab'), parts along dimension 0, may hold values from -6 to 6
- pressure_prev: float32 [4, 64, 64, 256], P('ens', 'box', 'slab'), parts along dimension 0, may hold values from -6 to 6
- courant_sq: float32 [64, 64, 256], P('box', 'slab'), may hold values from 0.04 to 0.28
- member_profiles: float32 [8, 64], replicated, may hold values from -0.15 to 0.15
- member_ids: int32 [4], P('ens'), parts along dimension 0, may hold values from 0 to 7, as said below
- stored_slabs: float32 [8, 16, 6144], P('slab'), may hold values from -6 to 6
- slab_home: int32 [2], P('ens'), parts along dimension 0, may hold values from 0 to 7
- interp_weights: float32 [2, 16], replicated, may hold values from -1.5 to 1.5
- surface_cells: int32 [6, 1024], replicated, may hold values from 0 to 1048575, as said below
Outputs:
- pressure_next: float32 [4, 64, 64, 256], P('ens', 'box', 'slab'), parts along dimension 0
- pressure_last: float32 [4, 64, 64, 256], P('ens', 'box', 'slab'), parts along dimension 0
The draws below stay inside these ranges and needn't reach their ends.
There are 2 independent parts, one for each index of `ens`. The reference program is written for one: setup_inputs(seed, part) draws one part's arguments, and reference() takes and returns one part's arrays. A program takes and returns all parts, laid end to end along the dimension named above; an argument that names none is the same for every part. Nothing has to cross between parts.
Inputs may be any that keep to these rules, and one draw needn't show every extreme that they name: `surface_cells`: row f lists 1024 cells, flat index (x 64 + z) * 256 + y, on one face of the box surface 0 cells inside the grid: x low, x high, z low, z high, y low, y high in this order; the other two coordinates lie on the surface; on every face other than the two depth faces, every depth of the surface occurs; cells may repeat. `slab_home`: block k is stored on the slab device k // 2, in its slot k % 2. `member_ids`: the members' profiles are all different.
All inputs are finite; a program needn't handle non-finite values.
Results may differ from the reference program's by a relative error of at most 0.000098.
Values sent between devices are 32-bit elements; how exact they have to be, the bound alone decides.
A program may use at most 64 MiB of HBM per device.

```python
import math
import jax
import jax.numpy as jnp
from jax import lax

MEMBERS = 2
STEPS = 2
SLAB_LEN = 16
BANK = 8
HUYGENS_GAP = 0
NY = 256
PTS_FACE = 1024
NX = 64
NZ = 64
BLOCKS = 8
POINTS = 6144


def draw_member_ids(key, part):
    order = jax.random.permutation(jax.random.fold_in(key, 29), jnp.arange(BANK, dtype=jnp.int32))
    return order[:MEMBERS].astype(jnp.int32)


def draw_surface_cells(key, part):
    subkeys = jax.random.split(jax.random.fold_in(key, 17), 4)
    face_index = jnp.arange(6, dtype=jnp.int32)[:, None]
    point_index = jnp.arange(PTS_FACE, dtype=jnp.int32)[None, :]
    along_x = jax.random.randint(subkeys[0], (6, PTS_FACE), HUYGENS_GAP, NX - HUYGENS_GAP)
    along_z = jax.random.randint(subkeys[1], (6, PTS_FACE), HUYGENS_GAP, NZ - HUYGENS_GAP)
    along_y = jax.random.randint(subkeys[2], (6, PTS_FACE), HUYGENS_GAP, NY - HUYGENS_GAP)
    depth_span = NZ - 2 * HUYGENS_GAP
    offset = jax.random.randint(subkeys[3], (6, 1), 0, depth_span)
    covering = HUYGENS_GAP + (point_index + offset) % depth_span
    along_z = jnp.where(point_index < depth_span, covering, along_z)
    along_x = jnp.where(face_index == 0, HUYGENS_GAP, jnp.where(face_index == 1, NX - 1 - HUYGENS_GAP, along_x))
    along_z = jnp.where(face_index == 2, HUYGENS_GAP, jnp.where(face_index == 3, NZ - 1 - HUYGENS_GAP, along_z))
    along_y = jnp.where(face_index == 4, HUYGENS_GAP, jnp.where(face_index == 5, NY - 1 - HUYGENS_GAP, along_y))
    return ((along_x * NZ + along_z) * NY + along_y).astype(jnp.int32)


def levels(own_key, extent, cuts, smallest, high):
    gain, own = 1.0, jax.random.fold_in(own_key, 6)
    for position, parts in cuts:
        heights = jnp.exp(jax.random.uniform(jax.random.fold_in(own, position), (parts,), jnp.float32, smallest / len(cuts), high / len(cuts)))
        gain = gain * jnp.repeat(heights, extent[position] // parts).reshape([-1 if axis == position else 1 for axis in range(len(extent))])
    return gain


def gaussian(rng, shape, width, reach, cuts=(), kind=jnp.bfloat16):
    values = jax.random.normal(rng, shape, jnp.float32) * width
    if len(cuts) > 0:
        values = levels(rng, shape, cuts, -0.22, 0.18) * values
    return jnp.clip(values, min=-reach, max=reach).astype(kind)


def setup_inputs(seed: int = 0, part: int = 0) -> dict:
    arg_keys = jax.random.split(jax.random.key(seed), 10)
    part_splits = jax.random.split(jax.random.fold_in(arg_keys[9], part), 10)
    pressure_now = gaussian(part_splits[0], (MEMBERS, NX, NZ, NY), 1.0, 6.0, ((1, 4), (2, 4)), jnp.float32)
    pressure_prev = gaussian(part_splits[1], (MEMBERS, NX, NZ, NY), 1.0, 6.0, ((1, 4), (2, 4)), jnp.float32)
    courant_sq = jnp.clip(jnp.exp(math.log(0.28) - 1.9459102 * jax.random.uniform(arg_keys[2], (NX, NZ, NY), jnp.float32) ** levels(arg_keys[2], (NX, NZ, NY), ((0, 4), (1, 4)), -0.2, 0.2)), 0.04, 0.28)
    member_profiles = jnp.clip(jax.random.uniform(arg_keys[3], (BANK, NZ), jnp.float32, -0.15, 0.15), -0.15, 0.15)
    member_ids = draw_member_ids(jax.random.fold_in(jax.random.fold_in(arg_keys[9], part), 71), part)
    stored_slabs = gaussian(arg_keys[5], (BLOCKS, SLAB_LEN, POINTS), 1.0, 6.0, ((0, 4),), jnp.float32)
    slab_home = jax.random.randint(part_splits[6], (1,), 0, BLOCKS).astype(jnp.int32)
    interp_weights = gaussian(arg_keys[7], (STEPS, SLAB_LEN), 0.3, 1.5, (), jnp.float32)
    surface_cells = draw_surface_cells(jax.random.fold_in(arg_keys[9], 71), part)
    return {"pressure_now": pressure_now, "pressure_prev": pressure_prev, "courant_sq": courant_sq, "member_profiles": member_profiles, "member_ids": member_ids, "stored_slabs": stored_slabs, "slab_home": slab_home, "interp_weights": interp_weights, "surface_cells": surface_cells}


def laplace(ext):
    inner = ext[:, 1:-1, 1:-1, :]
    beside = ext[:, 2:, 1:-1, :] + ext[:, :-2, 1:-1, :]
    beside = beside + ext[:, 1:-1, 2:, :] + ext[:, 1:-1, :-2, :]
    padded = jnp.pad(inner, ((0, 0), (0, 0), (0, 0), (1, 1)))
    beside = beside + padded[:, :, :, 2:] + padded[:, :, :, :-2]
    return beside - 6.0 * inner


def reference(pressure_now, pressure_prev, courant_sq, member_profiles, member_ids, stored_slabs, slab_home, interp_weights, surface_cells):
    profile = member_profiles[member_ids]
    coef = courant_sq[None] * (1.0 + profile[:, None, :, None])
    block = lax.dynamic_index_in_dim(stored_slabs, slab_home[0], 0, keepdims=False)
    values = jnp.dot(interp_weights, block, precision=lax.Precision.HIGHEST)
    cells = surface_cells.reshape(-1)
    prev, now = pressure_prev, pressure_now
    for step in range(STEPS):
        ext = jnp.pad(now, ((0, 0), (1, 1), (1, 1), (0, 0)))
        nxt = 2.0 * now - prev + coef * laplace(ext)
        source = jnp.zeros((NX * NZ * NY,), jnp.float32).at[cells].add(values[step])
        nxt = nxt + source.reshape(NX, NZ, NY)[None]
        prev, now = now, nxt
    return now, prev
```

```python
import functools

import jax
import jax.numpy as jnp
from jax import lax
from jax.experimental import pallas as pl
from jax.experimental.pallas import tpu as pltpu
from jax.sharding import PartitionSpec as P

F32, BF16, I32 = jnp.float32, jnp.bfloat16, jnp.int32
MESH = pl.DeviceIdType.MESH


def iota(shape, dim):
    return lax.broadcasted_iota(I32, shape, dim)


def quotient(values, divisor):
    if divisor & (divisor - 1) == 0:
        return lax.shift_right_logical(values, divisor.bit_length() - 1)
    return lax.div(values, jnp.full_like(values, divisor))


def split3(v):
    high = v.astype(BF16).astype(F32)
    rest = v - high
    mid = rest.astype(BF16).astype(F32)
    return high, mid, rest - mid


def place(rows, row_of, valid, per_step, cols, col_of):
    hit = (iota((rows, row_of.shape[1]), 0) == row_of) & valid
    parts = []
    for v in per_step:
        for term in split3(v):
            parts.append(jnp.where(hit, term, 0.0).astype(BF16))
    left = jnp.concatenate(parts, axis=0)
    right = jnp.where(iota((cols, col_of.shape[1]), 0) == col_of, 1.0, 0.0).astype(BF16)
    sums = lax.dot_general(left, right, (((1,), (1,)), ((), ())), preferred_element_type=F32)
    out = []
    for t in range(len(per_step)):
        a = sums[3 * t * rows : (3 * t + 1) * rows]
        b = sums[(3 * t + 1) * rows : (3 * t + 2) * rows]
        c = sums[(3 * t + 2) * rows : (3 * t + 3) * rows]
        out.append(a + (b + c))
    return out


def kernel(dims, ids, home, prof, weights, cells, now_h, prev_h, cour_h, slabs_h, two, one,
           now, prev, coef, slabs, zsend, xghost, zghost, vsend, vrecv,
           load_sem, hs_sem, hr_sem, vs_sem, vr_sem):
    members, wx, wz, ny, slots, length, pts, n_box, n_slab = dims
    steps = 2
    block = wx * wz
    box, slab = lax.axis_index("box"), lax.axis_index("slab")
    loads = [
        pltpu.make_async_copy(src, dst, load_sem.at[i])
        for i, (src, dst) in enumerate(((now_h, now), (slabs_h, slabs), (prev_h, prev), (cour_h, coef.at[pl.ds(0, block)])))
    ]
    for c in loads:
        c.start()

    barrier = pltpu.get_barrier_semaphore()

    def greet(target):
        pl.semaphore_signal(barrier, inc=1, device_id=target, device_id_type=MESH)

    @pl.when(box > 0)
    def _():
        greet({"box": box - 1})

    @pl.when(box < n_box - 1)
    def _():
        greet({"box": box + 1})

    for d in range(1, n_slab):
        greet({"slab": lax.rem(slab + d, n_slab)})
    box_peers = jnp.where(box > 0, 1, 0) + jnp.where(box < n_box - 1, 1, 0)
    pl.semaphore_wait(barrier, n_slab - 1 + box_peers)

    def halo(field, r, way):
        if way < 2:
            plane = wx - 1 if way == 0 else 0
            peer = {"box": box + 1 if way == 0 else box - 1}
            return [
                pltpu.make_async_remote_copy(
                    field.at[pl.ds((m * wx + plane) * wz, wz)], xghost.at[r, way, m],
                    hs_sem.at[r, way, m], hr_sem.at[r, way, m], device_id=peer, device_id_type=MESH)
                for m in range(members)
            ]
        peer = {"slab": slab + 1 if way == 2 else slab - 1}
        return [
            pltpu.make_async_remote_copy(
                zsend.at[r, way - 2], zghost.at[r, way - 2], hs_sem.at[r, way, 0], hr_sem.at[r, way, 0],
                device_id=peer, device_id_type=MESH)
        ]

    sends_to = (box < n_box - 1, box > 0, slab < n_slab - 1, slab > 0)
    hears_from = (box > 0, box < n_box - 1, slab > 0, slab < n_slab - 1)

    def send_halos(field, r):
        for way in (0, 1):
            @pl.when(sends_to[way])
            def _(way=way):
                for c in halo(field, r, way):
                    c.start()
        for way in (2, 3):
            row = wz - 1 if way == 2 else 0
            for m in range(members):
                for x in range(wx):
                    zsend[r, way - 2, m, x : x + 1, :] = field[pl.ds((m * wx + x) * wz + row, 1), :]

            @pl.when(sends_to[way])
            def _(way=way):
                for c in halo(field, r, way):
                    c.start()

    def add_halos(field, r, out):
        for way in (0, 1):
            plane = 0 if way == 0 else wx - 1

            @pl.when(hears_from[way])
            def _(way=way, plane=plane):
                for m, c in enumerate(halo(field, r, way)):
                    c.wait_recv()
                for m in range(members):
                    rows = pl.ds((m * wx + plane) * wz, wz)
                    out[rows, :] += coef[rows, :] * xghost[r, way, m]
        for way in (2, 3):
            row = 0 if way == 2 else wz - 1

            @pl.when(hears_from[way])
            def _(way=way, row=row):
                for c in halo(field, r, way):
                    c.wait_recv()
                for m in range(members):
                    for x in range(wx):
                        at = pl.ds((m * wx + x) * wz + row, 1)
                        out[at, :] += coef[at, :] * zghost[r, way - 2, m, x : x + 1, :]

    def end_sends(field, r):
        for way in range(4):
            @pl.when(sends_to[way])
            def _(way=way):
                for c in halo(field, r, way):
                    c.wait_send()

    loads[0].wait()
    send_halos(now, 0)

    loads[1].wait()
    eye = iota((length, length), 0) == iota((length, length), 1)
    cols = []
    for t in range(steps):
        col = jnp.sum(jnp.where(eye, weights[t : t + 1, :], 0.0), axis=1, keepdims=True)
        cols.append([jnp.where(home[0] == slab * slots + s, col, 0.0) for s in range(slots)])

    def offered(face, t):
        at = pl.ds(pl.multiple_of(face * pts, 128), pts)
        total = cols[t][0] * slabs[pl.ds(0, length), at]
        for s in range(1, slots):
            total = total + cols[t][s] * slabs[pl.ds(s * length, length), at]
        return jnp.sum(total, axis=0, keepdims=True)

    face_x = jnp.where(box == 0, 0, 1)
    face_z = jnp.where(slab == 0, 2, 3)
    common = [offered(f, t) for f in (face_x, 4, 5) for t in range(steps)]
    for kind in range(2):
        vsend[kind] = jnp.concatenate(common + [offered(2 + kind, t) for t in range(steps)], axis=0)

    def give(d):
        peer = lax.rem(slab + d, n_slab)
        return pltpu.make_async_remote_copy(
            vsend.at[jnp.where(peer == 0, 0, 1)], vrecv.at[d - 1], vs_sem.at[d - 1], vr_sem.at[d - 1],
            device_id={"slab": peer}, device_id_type=MESH)

    for d in range(1, n_slab):
        give(d).start()

    loads[3].wait()
    bank, total_z = prof.shape
    here = iota((wz, total_z), 1) == slab * wz + iota((wz, total_z), 0)
    for m in reversed(range(members)):
        mine = jnp.sum(jnp.where(iota((bank, total_z), 0) == ids[m], prof[...], 0.0), axis=0, keepdims=True)
        gain = 1.0 + jnp.sum(jnp.where(here, mine, 0.0), axis=1, keepdims=True)
        for x in range(wx):
            coef[pl.ds((m * wx + x) * wz, wz), :] = coef[pl.ds(x * wz, wz), :] * gain

    z_at, y_at = iota((wz, ny), 0), iota((wz, ny), 1)

    def advance(field, before, out):
        def member(m, carry):
            base = m * block
            for x in range(wx):
                rows = pl.ds(pl.multiple_of(base + x * wz, 8), wz)
                c = field[rows, :]
                lap = -6.0 * c
                if x > 0:
                    lap = lap + field[pl.ds(pl.multiple_of(base + (x - 1) * wz, 8), wz), :]
                if x < wx - 1:
                    lap = lap + field[pl.ds(pl.multiple_of(base + (x + 1) * wz, 8), wz), :]
                lap = lap + jnp.where(z_at == 0, 0.0, pltpu.roll(c, 1, 0))
                lap = lap + jnp.where(z_at == wz - 1, 0.0, pltpu.roll(c, wz - 1, 0))
                lap = lap + jnp.where(y_at == 0, 0.0, pltpu.roll(c, 1, 1))
                lap = lap + jnp.where(y_at == ny - 1, 0.0, pltpu.roll(c, ny - 1, 1))
                out[rows, :] = (2.0 * c - before[rows, :]) + coef[rows, :] * lap
            return carry

        lax.fori_loop(0, members, member, 0)

    loads[2].wait()
    advance(now, prev, one)

    def where_is(face):
        cell = cells[pl.ds(face, 1), :]
        cx = quotient(cell, total_z * ny)
        rest = cell - cx * (total_z * ny)
        cz = quotient(rest, ny)
        return cx - box * wx, cz - slab * wz, rest - cz * ny

    for d in range(1, n_slab):
        give(d).wait_recv()
    values = vsend[jnp.where(slab == 0, 0, 1)]
    for d in range(1, n_slab):
        values = values + vrecv[d - 1]

    def rows_of(k):
        return [values[2 * k + t : 2 * k + t + 1] for t in range(steps)]

    ax, az, ay = where_is(face_x)
    on_x = place(wz, az, (ax >= 0) & (ax < wx), rows_of(0), ny, ay)
    ax, az, ay = where_is(face_z)
    on_z = place(wx, ax, (az >= 0) & (az < wz), rows_of(3), ny, ay)
    wide = 128
    sides = []
    for k, face in ((1, 4), (2, 5)):
        ax, az, ay = where_is(face)
        sides.append(place(wz, az, (ax >= 0) & (ax < wx), rows_of(k), wide, ax))
    plane_x = jnp.where(box == 0, 0, wx - 1)
    row_z = jnp.where(slab == 0, 0, wz - 1)

    def add_source(t, out):
        lane = iota((wz, 128), 1)
        for x in range(wx):
            low = jnp.where(lane == 0, sides[0][t][:, x : x + 1], 0.0)
            high = jnp.where(lane == 127, sides[1][t][:, x : x + 1], 0.0)
            depth = jnp.where(z_at == row_z, on_z[t][x : x + 1, :], 0.0)
            for m in range(members):
                rows = pl.ds((m * wx + x) * wz, wz)
                out[rows, :] += depth
                out[rows, pl.ds(0, 128)] += low
                out[rows, pl.ds(ny - 128, 128)] += high
        for m in range(members):
            rows = pl.ds(pl.multiple_of((m * wx + plane_x) * wz, 8), wz)
            out[rows, :] += on_x[t]

    add_source(0, one)
    add_halos(now, 0, one)

    send_halos(one, 1)
    advance(one, now, two)
    add_source(1, two)
    add_halos(one, 1, two)
    end_sends(now, 0)
    end_sends(one, 1)
    for d in range(1, n_slab):
        give(d).wait_send()


def on_device(pressure_now, pressure_prev, courant_sq, member_profiles, member_ids, stored_slabs,
              slab_home, interp_weights, surface_cells):
    members, wx, wz, ny = pressure_now.shape
    slots, length, points = stored_slabs.shape
    pts = surface_cells.shape[1]
    n_box, n_slab = lax.axis_size("box"), lax.axis_size("slab")
    dims = (members, wx, wz, ny, slots, length, pts, n_box, n_slab)
    rows = members * wx * wz
    vmem = pl.BlockSpec(memory_space=pltpu.VMEM)
    smem = pl.BlockSpec(memory_space=pltpu.SMEM)
    hbm = pl.BlockSpec(memory_space=pltpu.HBM)
    field = jax.ShapeDtypeStruct((rows, ny), F32)
    dma = pltpu.SemaphoreType.DMA
    new, last = pl.pallas_call(
        functools.partial(kernel, dims),
        out_shape=(field, field),
        in_specs=[smem, smem, vmem, vmem, vmem, hbm, hbm, hbm, hbm],
        out_specs=(vmem, vmem),
        scratch_shapes=[pltpu.VMEM((rows, ny), F32)] * 3
        + [
            pltpu.VMEM((slots * length, points), F32),
            pltpu.VMEM((2, 2, members, wx, ny), F32),
            pltpu.VMEM((2, 2, members, wz, ny), F32),
            pltpu.VMEM((2, 2, members, wx, ny), F32),
            pltpu.VMEM((2, 8, pts), F32),
            pltpu.VMEM((n_slab - 1, 8, pts), F32),
            dma((4,)), dma((2, 4, members)), dma((2, 4, members)),
            dma((n_slab - 1,)), dma((n_slab - 1,)),
        ],
        compiler_params=pltpu.CompilerParams(collective_id=0, has_side_effects=True,
                                             vmem_limit_bytes=32 * 1024 * 1024),
    )(
        member_ids, slab_home, member_profiles, interp_weights, surface_cells,
        pressure_now.reshape(rows, ny), pressure_prev.reshape(rows, ny),
        courant_sq.reshape(wx * wz, ny), stored_slabs.reshape(slots * length, points),
    )
    return new.reshape(pressure_now.shape), last.reshape(pressure_now.shape)


def solution(mesh):
    in_specs = (
        P("ens", "box", "slab", None), P("ens", "box", "slab", None), P("box", "slab", None), P(),
        P("ens"), P("slab", None, None), P("ens"), P(), P(),
    )
    out_specs = (P("ens", "box", "slab", None), P("ens", "box", "slab", None))
    return jax.shard_map(on_device, mesh=mesh, in_specs=in_specs, out_specs=out_specs, check_vma=False)
```

```python
import functools

import jax
import jax.numpy as jnp
from jax import lax
from jax.experimental import pallas as pl
from jax.experimental.pallas import tpu as pltpu
from jax.sharding import PartitionSpec as P

F32, BF16, I32 = jnp.float32, jnp.bfloat16, jnp.int32
MESH = pl.DeviceIdType.MESH


def iota(shape, dim):
    return lax.broadcasted_iota(I32, shape, dim)


def quotient(values, divisor):
    if divisor & (divisor - 1) == 0:
        return lax.shift_right_logical(values, divisor.bit_length() - 1)
    return lax.div(values, jnp.full_like(values, divisor))


def split3(v):
    high = v.astype(BF16).astype(F32)
    rest = v - high
    mid = rest.astype(BF16).astype(F32)
    return high, mid, rest - mid


def place(rows, row_of, valid, per_step, right):
    hit = (iota((rows, row_of.shape[1]), 0) == row_of) & valid
    parts = []
    for v in per_step:
        for term in split3(v):
            parts.append(jnp.where(hit, term, 0.0).astype(BF16))
    left = jnp.concatenate(parts, axis=0)
    sums = lax.dot_general(left, right, (((1,), (1,)), ((), ())), preferred_element_type=F32)
    out = []
    for t in range(len(per_step)):
        a = sums[3 * t * rows : (3 * t + 1) * rows]
        b = sums[(3 * t + 1) * rows : (3 * t + 2) * rows]
        c = sums[(3 * t + 2) * rows : (3 * t + 3) * rows]
        out.append(a + (b + c))
    return out


def kernel(dims, home, ids_h, prof_h, weights_h, cells_h, now_h, prev_h, cour_h, slabs_h, two, one,
           ids, prof, weights, cells, now, prev, coef, slabs, xsend, zsend, xghost, zghost, xextra, zextra,
           hot_x, hot_z, hot_low, hot_high, vsend, vrecv, load_sem, hs_sem, hr_sem, vs_sem, vr_sem):
    members, wx, wz, ny, slots, length, pts, n_box, n_slab = dims
    steps = 2
    block = wx * wz
    box, slab = lax.axis_index("box"), lax.axis_index("slab")
    barrier = pltpu.get_barrier_semaphore()

    def greet(target):
        pl.semaphore_signal(barrier, inc=1, device_id=target, device_id_type=MESH)

    @pl.when(box > 0)
    def _():
        greet({"box": box - 1})

    @pl.when(box < n_box - 1)
    def _():
        greet({"box": box + 1})

    for d in range(1, n_slab):
        greet({"slab": lax.rem(slab + d, n_slab)})
    pairs = ((now_h, now), (slabs_h, slabs), (weights_h, weights), (cour_h, coef.at[pl.ds(0, block)]),
             (prof_h, prof), (ids_h, ids), (prev_h, prev), (cells_h, cells))
    loads = [pltpu.make_async_copy(src, dst, load_sem.at[i]) for i, (src, dst) in enumerate(pairs)]
    for c in loads:
        c.start()

    def source(r, way, m):
        if r > 0:
            return xsend.at[way, m]
        return now.at[pl.ds((m * wx + (wx - 1 if way == 0 else 0)) * wz, wz)]

    def halo(r, way):
        if way < 2:
            peer = {"box": box + 1 if way == 0 else box - 1}
            return [
                pltpu.make_async_remote_copy(
                    source(r, way, m), xghost.at[r, way, m],
                    hs_sem.at[r, way, m], hr_sem.at[r, way, m], device_id=peer, device_id_type=MESH)
                for m in range(members)
            ]
        peer = {"slab": slab + 1 if way == 2 else slab - 1}
        return [
            pltpu.make_async_remote_copy(
                zsend.at[r, way - 2], zghost.at[r, way - 2], hs_sem.at[r, way, 0], hr_sem.at[r, way, 0],
                device_id=peer, device_id_type=MESH)
        ]

    sends_to = (box < n_box - 1, box > 0, slab < n_slab - 1, slab > 0)
    hears_from = (box > 0, box < n_box - 1, slab > 0, slab < n_slab - 1)

    def pack(field, r):
        for m in range(members):
            if r > 0:
                for way in (0, 1):
                    plane = wx - 1 if way == 0 else 0
                    xsend[way, m] = field[pl.ds((m * wx + plane) * wz, wz), :]
            for way in (2, 3):
                row = wz - 1 if way == 2 else 0
                for x in range(wx):
                    zsend[r, way - 2, m, x : x + 1, :] = field[pl.ds((m * wx + x) * wz + row, 1), :]

    def send_halos(r):
        for way in range(4):
            @pl.when(sends_to[way])
            def _(way=way):
                for c in halo(r, way):
                    c.start()

    def add_halos(r, out):
        for way in (0, 1):
            plane = 0 if way == 0 else wx - 1

            @pl.when(hears_from[way])
            def _(way=way, plane=plane):
                for m, c in enumerate(halo(r, way)):
                    c.wait_recv()
                for m in range(members):
                    rows = pl.ds((m * wx + plane) * wz, wz)
                    ghost = xghost[r, way, m]
                    if r > 0:
                        ghost = ghost + xextra[way]
                    out[rows, :] += coef[rows, :] * ghost
        for way in (2, 3):
            row = 0 if way == 2 else wz - 1

            @pl.when(hears_from[way])
            def _(way=way, row=row):
                for c in halo(r, way):
                    c.wait_recv()
                for m in range(members):
                    for x in range(wx):
                        at = pl.ds((m * wx + x) * wz + row, 1)
                        ghost = zghost[r, way - 2, m, x : x + 1, :]
                        if r > 0:
                            ghost = ghost + zextra[way - 2, x : x + 1, :]
                        out[at, :] += coef[at, :] * ghost

    def end_sends(r):
        for way in range(4):
            @pl.when(sends_to[way])
            def _(way=way):
                for c in halo(r, way):
                    c.wait_send()

    loads[0].wait()
    pack(now, 0)
    box_peers = jnp.where(box > 0, 1, 0) + jnp.where(box < n_box - 1, 1, 0)
    pl.semaphore_wait(barrier, n_slab - 1 + box_peers)
    send_halos(0)

    for i in (1, 2):
        loads[i].wait()
    eye = iota((length, length), 0) == iota((length, length), 1)
    cols = []
    for t in range(steps):
        col = jnp.sum(jnp.where(eye, weights[t : t + 1, :], 0.0), axis=1, keepdims=True)
        cols.append([jnp.where(home[0] == slab * slots + s, col, 0.0) for s in range(slots)])

    def offered(face, t):
        at = pl.ds(pl.multiple_of(face * pts, 128), pts)
        total = cols[t][0] * slabs[pl.ds(0, length), at]
        for s in range(1, slots):
            total = total + cols[t][s] * slabs[pl.ds(s * length, length), at]
        return jnp.sum(total, axis=0, keepdims=True)

    face_x = jnp.where(box == 0, 0, 1)
    face_z = jnp.where(slab == 0, 2, 3)
    common = [offered(f, t) for f in (face_x, 4, 5) for t in range(steps)]
    for kind in range(2):
        vsend[kind] = jnp.concatenate(common + [offered(2 + kind, t) for t in range(steps)], axis=0)

    def give(d):
        peer = lax.rem(slab + d, n_slab)
        return pltpu.make_async_remote_copy(
            vsend.at[jnp.where(peer == 0, 0, 1)], vrecv.at[d - 1], vs_sem.at[d - 1], vr_sem.at[d - 1],
            device_id={"slab": peer}, device_id_type=MESH)

    for d in range(1, n_slab):
        give(d).start()

    for i in (3, 4, 5):
        loads[i].wait()
    bank, total_z = prof.shape
    here = iota((wz, total_z), 1) == slab * wz + iota((wz, total_z), 0)
    for m in reversed(range(members)):
        mine = jnp.sum(jnp.where(iota((bank, total_z), 0) == ids[m], prof[...], 0.0), axis=0, keepdims=True)
        gain = 1.0 + jnp.sum(jnp.where(here, mine, 0.0), axis=1, keepdims=True)
        for x in range(wx):
            coef[pl.ds((m * wx + x) * wz, wz), :] = coef[pl.ds(x * wz, wz), :] * gain

    z_at, y_at = iota((wz, ny), 0), iota((wz, ny), 1)

    def advance(field, before, out):
        def member(m, carry):
            base = m * block
            for x in range(wx):
                rows = pl.ds(pl.multiple_of(base + x * wz, 8), wz)
                c = field[rows, :]
                lap = -6.0 * c
                if x > 0:
                    lap = lap + field[pl.ds(pl.multiple_of(base + (x - 1) * wz, 8), wz), :]
                if x < wx - 1:
                    lap = lap + field[pl.ds(pl.multiple_of(base + (x + 1) * wz, 8), wz), :]
                lap = lap + jnp.where(z_at == 0, 0.0, pltpu.roll(c, 1, 0))
                lap = lap + jnp.where(z_at == wz - 1, 0.0, pltpu.roll(c, wz - 1, 0))
                lap = lap + jnp.where(y_at == 0, 0.0, pltpu.roll(c, 1, 1))
                lap = lap + jnp.where(y_at == ny - 1, 0.0, pltpu.roll(c, ny - 1, 1))
                out[rows, :] = (2.0 * c - before[rows, :]) + coef[rows, :] * lap
            return carry

        lax.fori_loop(0, members, member, 0)

    loads[6].wait()
    advance(now, prev, one)

    loads[7].wait()
    margin, wide = 8, 128

    def where_is(face):
        cell = cells[pl.ds(face, 1), :]
        cx = quotient(cell, total_z * ny)
        rest = cell - cx * (total_z * ny)
        cz = quotient(rest, ny)
        return cx - box * wx, cz - slab * wz, rest - cz * ny

    def hot(cols, col_of):
        return jnp.where(iota((cols, pts), 0) == col_of, 1.0, 0.0).astype(BF16)

    px, pz, py = where_is(face_x)
    px_valid = (px >= 0) & (px < wx)
    px_row = pz + margin
    hot_x[...] = hot(ny, py)
    px, pz, py = where_is(face_z)
    pz_valid = (pz >= 0) & (pz < wz)
    pz_row = px + margin
    hot_z[...] = hot(ny, py)
    px, pz, py = where_is(4)
    low_row = pz + margin
    hot_low[...] = hot(wide, px + margin)
    px, pz, py = where_is(5)
    high_row = pz + margin
    hot_high[...] = hot(wide, px + margin)

    add_halos(0, one)
    pack(one, 1)
    send_halos(1)

    for d in range(1, n_slab):
        give(d).wait_recv()
    values = vsend[jnp.where(slab == 0, 0, 1)]
    for d in range(1, n_slab):
        values = values + vrecv[d - 1]

    def rows_of(k):
        return [values[2 * k + t : 2 * k + t + 1] for t in range(steps)]

    tall_x, tall_z = wx + 2 * margin, wz + 2 * margin
    always = low_row >= -tall_z * n_slab * pts
    on_x = place(tall_z, px_row, px_valid, rows_of(0), hot_x[...])
    on_z = place(tall_x, pz_row, pz_valid, rows_of(3), hot_z[...])
    low_y = place(tall_z, low_row, always, rows_of(1), hot_low[...])
    high_y = place(tall_z, high_row, always, rows_of(2), hot_high[...])
    plane_x = jnp.where(box == 0, 0, wx - 1)
    row_z = jnp.where(slab == 0, 0, wz - 1) + margin
    tall_row, tall_lane = iota((tall_z, ny), 0), iota((tall_z, ny), 1)

    def source_plane(t, x):
        at = x + margin
        out = jnp.where(tall_row == row_z, on_z[t][at : at + 1, :], 0.0)
        out = out + jnp.where(tall_lane == 0, low_y[t][:, at : at + 1], 0.0)
        out = out + jnp.where(tall_lane == ny - 1, high_y[t][:, at : at + 1], 0.0)
        if x in (0, wx - 1):
            out = out + jnp.where(plane_x == x, on_x[t], 0.0)
        return out

    def add_source(t, out):
        for x in range(wx):
            plane = source_plane(t, x)
            if t == 0:
                zextra[0, x : x + 1, :] = plane[margin - 1 : margin]
                zextra[1, x : x + 1, :] = plane[margin + wz : margin + wz + 1]
            for m in range(members):
                out[pl.ds((m * wx + x) * wz, wz), :] += plane[margin : margin + wz]
        if t == 0:
            xextra[0] = source_plane(t, -1)[margin : margin + wz]
            xextra[1] = source_plane(t, wx)[margin : margin + wz]

    add_source(0, one)
    advance(one, now, two)
    add_source(1, two)
    add_halos(1, two)
    end_sends(0)
    end_sends(1)
    for d in range(1, n_slab):
        give(d).wait_send()


def on_device(pressure_now, pressure_prev, courant_sq, member_profiles, member_ids, stored_slabs,
              slab_home, interp_weights, surface_cells):
    members, wx, wz, ny = pressure_now.shape
    slots, length, points = stored_slabs.shape
    pts = surface_cells.shape[1]
    n_box, n_slab = lax.axis_size("box"), lax.axis_size("slab")
    dims = (members, wx, wz, ny, slots, length, pts, n_box, n_slab)
    rows = members * wx * wz
    vmem = pl.BlockSpec(memory_space=pltpu.VMEM)
    in_hbm = lambda a: pltpu.with_memory_space_constraint(a, pltpu.HBM)
    hbm = pl.BlockSpec(memory_space=pltpu.HBM)
    field = jax.ShapeDtypeStruct((rows, ny), F32)
    dma = pltpu.SemaphoreType.DMA
    new, last = pl.pallas_call(
        functools.partial(kernel, dims),
        out_shape=(field, field),
        in_specs=[pl.BlockSpec(memory_space=pltpu.SMEM)] + [hbm] * 8,
        out_specs=(vmem, vmem),
        scratch_shapes=[
            pltpu.SMEM(member_ids.shape, I32),
            pltpu.VMEM(member_profiles.shape, F32), pltpu.VMEM(interp_weights.shape, F32),
            pltpu.VMEM(surface_cells.shape, I32),
            pltpu.VMEM((rows, ny), F32), pltpu.VMEM((rows, ny), F32), pltpu.VMEM((rows, ny), F32),
            pltpu.VMEM((slots * length, points), F32),
            pltpu.VMEM((2, members, wz, ny), F32),
            pltpu.VMEM((2, 2, members, wx, ny), F32),
            pltpu.VMEM((2, 2, members, wz, ny), F32),
            pltpu.VMEM((2, 2, members, wx, ny), F32),
            pltpu.VMEM((2, wz, ny), F32), pltpu.VMEM((2, wx, ny), F32),
            pltpu.VMEM((ny, pts), BF16), pltpu.VMEM((ny, pts), BF16),
            pltpu.VMEM((128, pts), BF16), pltpu.VMEM((128, pts), BF16),
            pltpu.VMEM((2, 8, pts), F32),
            pltpu.VMEM((n_slab - 1, 8, pts), F32),
            dma((8,)), dma((2, 4, members)), dma((2, 4, members)),
            dma((n_slab - 1,)), dma((n_slab - 1,)),
        ],
        compiler_params=pltpu.CompilerParams(collective_id=0, has_side_effects=True,
                                             vmem_limit_bytes=32 * 1024 * 1024),
    )(slab_home, *(in_hbm(a) for a in (
        member_ids, member_profiles, interp_weights, surface_cells,
        pressure_now.reshape(rows, ny), pressure_prev.reshape(rows, ny),
        courant_sq.reshape(wx * wz, ny), stored_slabs.reshape(slots * length, points),
    )))
    return new.reshape(pressure_now.shape), last.reshape(pressure_now.shape)


def solution(mesh):
    in_specs = (
        P("ens", "box", "slab", None), P("ens", "box", "slab", None), P("box", "slab", None), P(),
        P("ens"), P("slab", None, None), P("ens"), P(), P(),
    )
    out_specs = (P("ens", "box", "slab", None), P("ens", "box", "slab", None))
    return jax.shard_map(on_device, mesh=mesh, in_specs=in_specs, out_specs=out_specs, check_vma=False)
```

```python
import functools

import jax
import jax.numpy as jnp
from jax import lax
from jax.experimental import pallas as pl
from jax.experimental.pallas import tpu as pltpu
from jax.sharding import PartitionSpec as P

F32, BF16, I32 = jnp.float32, jnp.bfloat16, jnp.int32
MESH = pl.DeviceIdType.MESH


def iota(shape, dim):
    return lax.broadcasted_iota(I32, shape, dim)


def quotient(values, divisor):
    if divisor & (divisor - 1) == 0:
        return lax.shift_right_logical(values, divisor.bit_length() - 1)
    return lax.div(values, jnp.full_like(values, divisor))


def split3(v):
    high = v.astype(BF16).astype(F32)
    rest = v - high
    mid = rest.astype(BF16).astype(F32)
    return high, mid, rest - mid


def place(rows, row_of, valid, per_step, right):
    hit = (iota((rows, row_of.shape[1]), 0) == row_of) & valid
    parts = []
    for v in per_step:
        for term in split3(v):
            parts.append(jnp.where(hit, term, 0.0).astype(BF16))
    left = jnp.concatenate(parts, axis=0)
    sums = lax.dot_general(left, right, (((1,), (1,)), ((), ())), preferred_element_type=F32)
    out = []
    for t in range(len(per_step)):
        a = sums[3 * t * rows : (3 * t + 1) * rows]
        b = sums[(3 * t + 1) * rows : (3 * t + 2) * rows]
        c = sums[(3 * t + 2) * rows : (3 * t + 3) * rows]
        out.append(a + (b + c))
    return out


def kernel(dims, home, ids_h, prof_h, weights_h, cells_h, now_h, prev_h, cour_h, slabs_h, two, one,
           ids, prof, weights, cells, now, prev, coef, slabs, xsend, zsend, xghost, zghost, xextra, zextra,
           hot_x, hot_z, hot_low, hot_high, vsend, vrecv, load_sem, hs_sem, hr_sem, vs_sem, vr_sem):
    members, wx, wz, ny, slots, length, pts, n_box, n_slab = dims
    steps = 2
    block = wx * wz
    box, slab = lax.axis_index("box"), lax.axis_index("slab")
    pairs = ((now_h, now), (slabs_h, slabs), (weights_h, weights), (cour_h, coef.at[pl.ds(0, block)]),
             (prof_h, prof), (ids_h, ids), (prev_h, prev), (cells_h, cells))
    loads = [pltpu.make_async_copy(src, dst, load_sem.at[i]) for i, (src, dst) in enumerate(pairs)]
    loads[0].start()

    barrier = pltpu.get_barrier_semaphore()

    def greet(target):
        pl.semaphore_signal(barrier, inc=1, device_id=target, device_id_type=MESH)

    @pl.when(box > 0)
    def _():
        greet({"box": box - 1})

    @pl.when(box < n_box - 1)
    def _():
        greet({"box": box + 1})

    for d in range(1, n_slab):
        greet({"slab": lax.rem(slab + d, n_slab)})
    for c in loads[1:]:
        c.start()

    def source(r, way, m):
        if r > 0:
            return xsend.at[way, m]
        return now.at[pl.ds((m * wx + (wx - 1 if way == 0 else 0)) * wz, wz)]

    def halo(r, way):
        if way < 2:
            peer = {"box": box + 1 if way == 0 else box - 1}
            return [
                pltpu.make_async_remote_copy(
                    source(r, way, m), xghost.at[r, way, m],
                    hs_sem.at[r, way, m], hr_sem.at[r, way, m], device_id=peer, device_id_type=MESH)
                for m in range(members)
            ]
        peer = {"slab": slab + 1 if way == 2 else slab - 1}
        return [
            pltpu.make_async_remote_copy(
                zsend.at[r, way - 2], zghost.at[r, way - 2], hs_sem.at[r, way, 0], hr_sem.at[r, way, 0],
                device_id=peer, device_id_type=MESH)
        ]

    sends_to = (box < n_box - 1, box > 0, slab < n_slab - 1, slab > 0)
    hears_from = (box > 0, box < n_box - 1, slab > 0, slab < n_slab - 1)

    def pack(field, r):
        for m in range(members):
            if r > 0:
                for way in (0, 1):
                    plane = wx - 1 if way == 0 else 0
                    xsend[way, m] = field[pl.ds((m * wx + plane) * wz, wz), :]
            for way in (2, 3):
                row = wz - 1 if way == 2 else 0
                for x in range(wx):
                    zsend[r, way - 2, m, x : x + 1, :] = field[pl.ds((m * wx + x) * wz + row, 1), :]

    def send_halos(r):
        for way in range(4):
            @pl.when(sends_to[way])
            def _(way=way):
                for c in halo(r, way):
                    c.start()

    def add_halos(r, out):
        for way in (0, 1):
            plane = 0 if way == 0 else wx - 1

            @pl.when(hears_from[way])
            def _(way=way, plane=plane):
                for m, c in enumerate(halo(r, way)):
                    c.wait_recv()
                for m in range(members):
                    rows = pl.ds((m * wx + plane) * wz, wz)
                    ghost = xghost[r, way, m]
                    if r > 0:
                        ghost = ghost + xextra[way]
                    out[rows, :] += coef[rows, :] * ghost
        for way in (2, 3):
            row = 0 if way == 2 else wz - 1

            @pl.when(hears_from[way])
            def _(way=way, row=row):
                for c in halo(r, way):
                    c.wait_recv()
                for m in range(members):
                    for x in range(wx):
                        at = pl.ds((m * wx + x) * wz + row, 1)
                        ghost = zghost[r, way - 2, m, x : x + 1, :]
                        if r > 0:
                            ghost = ghost + zextra[way - 2, x : x + 1, :]
                        out[at, :] += coef[at, :] * ghost

    def end_sends(r):
        for way in range(4):
            @pl.when(sends_to[way])
            def _(way=way):
                for c in halo(r, way):
                    c.wait_send()

    loads[0].wait()
    pack(now, 0)
    box_peers = jnp.where(box > 0, 1, 0) + jnp.where(box < n_box - 1, 1, 0)
    pl.semaphore_wait(barrier, n_slab - 1 + box_peers)
    send_halos(0)

    for i in (1, 2):
        loads[i].wait()
    eye = iota((length, length), 0) == iota((length, length), 1)
    cols = []
    for t in range(steps):
        col = jnp.sum(jnp.where(eye, weights[t : t + 1, :], 0.0), axis=1, keepdims=True)
        cols.append([jnp.where(home[0] == slab * slots + s, col, 0.0) for s in range(slots)])

    def offered(face, t):
        at = pl.ds(pl.multiple_of(face * pts, 128), pts)
        total = cols[t][0] * slabs[pl.ds(0, length), at]
        for s in range(1, slots):
            total = total + cols[t][s] * slabs[pl.ds(s * length, length), at]
        return jnp.sum(total, axis=0, keepdims=True)

    face_x = jnp.where(box == 0, 0, 1)
    face_z = jnp.where(slab == 0, 2, 3)
    common = [offered(f, t) for f in (face_x, 4, 5) for t in range(steps)]
    for kind in range(2):
        vsend[kind] = jnp.concatenate(common + [offered(2 + kind, t) for t in range(steps)], axis=0)

    def give(d):
        peer = lax.rem(slab + d, n_slab)
        return pltpu.make_async_remote_copy(
            vsend.at[jnp.where(peer == 0, 0, 1)], vrecv.at[d - 1], vs_sem.at[d - 1], vr_sem.at[d - 1],
            device_id={"slab": peer}, device_id_type=MESH)

    for d in range(1, n_slab):
        give(d).start()

    for i in (3, 4, 5):
        loads[i].wait()
    bank, total_z = prof.shape
    here = iota((wz, total_z), 1) == slab * wz + iota((wz, total_z), 0)
    for m in reversed(range(members)):
        mine = jnp.sum(jnp.where(iota((bank, total_z), 0) == ids[m], prof[...], 0.0), axis=0, keepdims=True)
        gain = 1.0 + jnp.sum(jnp.where(here, mine, 0.0), axis=1, keepdims=True)
        for x in range(wx):
            coef[pl.ds((m * wx + x) * wz, wz), :] = coef[pl.ds(x * wz, wz), :] * gain

    z_at, y_at = iota((wz, ny), 0), iota((wz, ny), 1)

    def advance(field, before, out):
        def member(m, carry):
            base = m * block
            for x in range(wx):
                rows = pl.ds(pl.multiple_of(base + x * wz, 8), wz)
                c = field[rows, :]
                lap = -6.0 * c
                if x > 0:
                    lap = lap + field[pl.ds(pl.multiple_of(base + (x - 1) * wz, 8), wz), :]
                if x < wx - 1:
                    lap = lap + field[pl.ds(pl.multiple_of(base + (x + 1) * wz, 8), wz), :]
                lap = lap + jnp.where(z_at == 0, 0.0, pltpu.roll(c, 1, 0))
                lap = lap + jnp.where(z_at == wz - 1, 0.0, pltpu.roll(c, wz - 1, 0))
                lap = lap + jnp.where(y_at == 0, 0.0, pltpu.roll(c, 1, 1))
                lap = lap + jnp.where(y_at == ny - 1, 0.0, pltpu.roll(c, ny - 1, 1))
                out[rows, :] = (2.0 * c - before[rows, :]) + coef[rows, :] * lap
            return carry

        lax.fori_loop(0, members, member, 0)

    loads[6].wait()
    advance(now, prev, one)

    loads[7].wait()
    margin, wide = 8, 128

    def where_is(face):
        cell = cells[pl.ds(face, 1), :]
        cx = quotient(cell, total_z * ny)
        rest = cell - cx * (total_z * ny)
        cz = quotient(rest, ny)
        return cx - box * wx, cz - slab * wz, rest - cz * ny

    def hot(cols, col_of):
        return jnp.where(iota((cols, pts), 0) == col_of, 1.0, 0.0).astype(BF16)

    px, pz, py = where_is(face_x)
    px_valid = (px >= 0) & (px < wx)
    px_row = pz + margin
    hot_x[...] = hot(ny, py)
    px, pz, py = where_is(face_z)
    pz_valid = (pz >= 0) & (pz < wz)
    pz_row = px + margin
    hot_z[...] = hot(ny, py)
    px, pz, py = where_is(4)
    low_row = pz + margin
    hot_low[...] = hot(wide, px + margin)
    px, pz, py = where_is(5)
    high_row = pz + margin
    hot_high[...] = hot(wide, px + margin)

    add_halos(0, one)
    pack(one, 1)
    send_halos(1)

    for d in range(1, n_slab):
        give(d).wait_recv()
    values = vsend[jnp.where(slab == 0, 0, 1)]
    for d in range(1, n_slab):
        values = values + vrecv[d - 1]

    def rows_of(k):
        return [values[2 * k + t : 2 * k + t + 1] for t in range(steps)]

    tall_x, tall_z = wx + 2 * margin, wz + 2 * margin
    always = low_row >= -tall_z * n_slab * pts
    on_x = place(tall_z, px_row, px_valid, rows_of(0), hot_x[...])
    on_z = place(tall_x, pz_row, pz_valid, rows_of(3), hot_z[...])
    low_y = place(tall_z, low_row, always, rows_of(1), hot_low[...])
    high_y = place(tall_z, high_row, always, rows_of(2), hot_high[...])
    plane_x = jnp.where(box == 0, 0, wx - 1)
    row_z = jnp.where(slab == 0, 0, wz - 1) + margin
    tall_row, tall_lane = iota((tall_z, ny), 0), iota((tall_z, ny), 1)

    def source_plane(t, x):
        at = x + margin
        out = jnp.where(tall_row == row_z, on_z[t][at : at + 1, :], 0.0)
        out = out + jnp.where(tall_lane == 0, low_y[t][:, at : at + 1], 0.0)
        out = out + jnp.where(tall_lane == ny - 1, high_y[t][:, at : at + 1], 0.0)
        if x in (0, wx - 1):
            out = out + jnp.where(plane_x == x, on_x[t], 0.0)
        return out

    def add_source(t, out):
        for x in range(wx):
            plane = source_plane(t, x)
            if t == 0:
                zextra[0, x : x + 1, :] = plane[margin - 1 : margin]
                zextra[1, x : x + 1, :] = plane[margin + wz : margin + wz + 1]
            for m in range(members):
                out[pl.ds((m * wx + x) * wz, wz), :] += plane[margin : margin + wz]
        if t == 0:
            xextra[0] = source_plane(t, -1)[margin : margin + wz]
            xextra[1] = source_plane(t, wx)[margin : margin + wz]

    add_source(0, one)
    advance(one, now, two)
    add_source(1, two)
    add_halos(1, two)
    end_sends(0)
    end_sends(1)
    for d in range(1, n_slab):
        give(d).wait_send()


def store_kernel(two, one, next_h, last_h, sem):
    copies = [pltpu.make_async_copy(src, dst, sem.at[i]) for i, (src, dst) in enumerate(((two, next_h), (one, last_h)))]
    for c in copies:
        c.start()
    for c in copies:
        c.wait()


def on_device(pressure_now, pressure_prev, courant_sq, member_profiles, member_ids, stored_slabs,
              slab_home, interp_weights, surface_cells):
    members, wx, wz, ny = pressure_now.shape
    slots, length, points = stored_slabs.shape
    pts = surface_cells.shape[1]
    n_box, n_slab = lax.axis_size("box"), lax.axis_size("slab")
    dims = (members, wx, wz, ny, slots, length, pts, n_box, n_slab)
    rows = members * wx * wz
    vmem = pl.BlockSpec(memory_space=pltpu.VMEM)
    in_hbm = lambda a: pltpu.with_memory_space_constraint(a, pltpu.HBM)
    hbm = pl.BlockSpec(memory_space=pltpu.HBM)
    field = jax.ShapeDtypeStruct((rows, ny), F32)
    dma = pltpu.SemaphoreType.DMA
    new, last = pl.pallas_call(
        functools.partial(kernel, dims),
        out_shape=(field, field),
        in_specs=[pl.BlockSpec(memory_space=pltpu.SMEM)] + [hbm] * 8,
        out_specs=(vmem, vmem),
        scratch_shapes=[
            pltpu.SMEM(member_ids.shape, I32),
            pltpu.VMEM(member_profiles.shape, F32), pltpu.VMEM(interp_weights.shape, F32),
            pltpu.VMEM(surface_cells.shape, I32),
            pltpu.VMEM((rows, ny), F32), pltpu.VMEM((rows, ny), F32), pltpu.VMEM((rows, ny), F32),
            pltpu.VMEM((slots * length, points), F32),
            pltpu.VMEM((2, members, wz, ny), F32),
            pltpu.VMEM((2, 2, members, wx, ny), F32),
            pltpu.VMEM((2, 2, members, wz, ny), F32),
            pltpu.VMEM((2, 2, members, wx, ny), F32),
            pltpu.VMEM((2, wz, ny), F32), pltpu.VMEM((2, wx, ny), F32),
            pltpu.VMEM((ny, pts), BF16), pltpu.VMEM((ny, pts), BF16),
            pltpu.VMEM((128, pts), BF16), pltpu.VMEM((128, pts), BF16),
            pltpu.VMEM((2, 8, pts), F32),
            pltpu.VMEM((n_slab - 1, 8, pts), F32),
            dma((8,)), dma((2, 4, members)), dma((2, 4, members)),
            dma((n_slab - 1,)), dma((n_slab - 1,)),
        ],
        compiler_params=pltpu.CompilerParams(collective_id=0, has_side_effects=True,
                                             vmem_limit_bytes=32 * 1024 * 1024),
    )(slab_home, *(in_hbm(a) for a in (
        member_ids, member_profiles, interp_weights, surface_cells,
        pressure_now.reshape(rows, ny), pressure_prev.reshape(rows, ny),
        courant_sq.reshape(wx * wz, ny), stored_slabs.reshape(slots * length, points),
    )))
    placed = pltpu.HBM((rows, ny), F32)
    new, last = pl.pallas_call(
        store_kernel,
        out_shape=(placed, placed),
        in_specs=[vmem, vmem],
        out_specs=(hbm, hbm),
        scratch_shapes=[dma((2,))],
        compiler_params=pltpu.CompilerParams(vmem_limit_bytes=4 * 1024 * 1024),
    )(new, last)
    return new.reshape(pressure_now.shape), last.reshape(pressure_now.shape)


def solution(mesh):
    in_specs = (
        P("ens", "box", "slab", None), P("ens", "box", "slab", None), P("box", "slab", None), P(),
        P("ens"), P("slab", None, None), P("ens"), P(), P(),
    )
    out_specs = (P("ens", "box", "slab", None), P("ens", "box", "slab", None))
    return jax.shard_map(on_device, mesh=mesh, in_specs=in_specs, out_specs=out_specs, check_vma=False)
```

```python
import functools

import jax
import jax.numpy as jnp
from jax import lax
from jax.experimental import pallas as pl
from jax.experimental.pallas import tpu as pltpu
from jax.sharding import PartitionSpec as P

F32, BF16, I32 = jnp.float32, jnp.bfloat16, jnp.int32
MESH = pl.DeviceIdType.MESH


def iota(shape, dim):
    return lax.broadcasted_iota(I32, shape, dim)


def quotient(values, divisor):
    if divisor & (divisor - 1) == 0:
        return lax.shift_right_logical(values, divisor.bit_length() - 1)
    return lax.div(values, jnp.full_like(values, divisor))


def split3(v):
    high = v.astype(BF16).astype(F32)
    rest = v - high
    mid = rest.astype(BF16).astype(F32)
    return high, mid, rest - mid


def place(rows, row_of, valid, per_step, right):
    hit = (iota((rows, row_of.shape[1]), 0) == row_of) & valid
    parts = []
    for v in per_step:
        for term in split3(v):
            parts.append(jnp.where(hit, term, 0.0).astype(BF16))
    left = jnp.concatenate(parts, axis=0)
    sums = lax.dot_general(left, right, (((1,), (1,)), ((), ())), preferred_element_type=F32)
    out = []
    for t in range(len(per_step)):
        a = sums[3 * t * rows : (3 * t + 1) * rows]
        b = sums[(3 * t + 1) * rows : (3 * t + 2) * rows]
        c = sums[(3 * t + 2) * rows : (3 * t + 3) * rows]
        out.append(a + (b + c))
    return out


def kernel(dims, home, ids_h, prof_h, weights_h, cells_h, now_h, prev_h, cour_h, slabs_h, two, one,
           ids, prof, weights, cells, now, prev, coef, slabs, xsend, zsend, xghost, zghost, xextra, zextra,
           hot_x, hot_z, hot_low, hot_high, vsend, vrecv, load_sem, hs_sem, hr_sem, vs_sem, vr_sem):
    members, wx, wz, ny, slots, length, pts, n_box, n_slab = dims
    steps = 2
    block = wx * wz
    box, slab = lax.axis_index("box"), lax.axis_index("slab")
    pairs = ((now_h, now), (slabs_h, slabs), (weights_h, weights), (cour_h, coef.at[pl.ds(0, block)]),
             (prof_h, prof), (ids_h, ids), (prev_h, prev), (cells_h, cells))
    loads = [pltpu.make_async_copy(src, dst, load_sem.at[i]) for i, (src, dst) in enumerate(pairs)]
    loads[0].start()

    barrier = pltpu.get_barrier_semaphore()

    def greet(target):
        pl.semaphore_signal(barrier, inc=1, device_id=target, device_id_type=MESH)

    @pl.when(box > 0)
    def _():
        greet({"box": box - 1})

    @pl.when(box < n_box - 1)
    def _():
        greet({"box": box + 1})

    for d in range(1, n_slab):
        greet({"slab": lax.rem(slab + d, n_slab)})
    for i in (1, 2):
        loads[i].start()

    def source(r, way, m):
        if r > 0:
            return xsend.at[way, m]
        return now.at[pl.ds((m * wx + (wx - 1 if way == 0 else 0)) * wz, wz)]

    def halo(r, way):
        if way < 2:
            peer = {"box": box + 1 if way == 0 else box - 1}
            return [
                pltpu.make_async_remote_copy(
                    source(r, way, m), xghost.at[r, way, m],
                    hs_sem.at[r, way, m], hr_sem.at[r, way, m], device_id=peer, device_id_type=MESH)
                for m in range(members)
            ]
        peer = {"slab": slab + 1 if way == 2 else slab - 1}
        return [
            pltpu.make_async_remote_copy(
                zsend.at[r, way - 2], zghost.at[r, way - 2], hs_sem.at[r, way, 0], hr_sem.at[r, way, 0],
                device_id=peer, device_id_type=MESH)
        ]

    sends_to = (box < n_box - 1, box > 0, slab < n_slab - 1, slab > 0)
    hears_from = (box > 0, box < n_box - 1, slab > 0, slab < n_slab - 1)

    def pack(field, r):
        for m in range(members):
            if r > 0:
                for way in (0, 1):
                    plane = wx - 1 if way == 0 else 0
                    xsend[way, m] = field[pl.ds((m * wx + plane) * wz, wz), :]
            for way in (2, 3):
                row = wz - 1 if way == 2 else 0
                for x in range(wx):
                    zsend[r, way - 2, m, x : x + 1, :] = field[pl.ds((m * wx + x) * wz + row, 1), :]

    def send_halos(r):
        for way in range(4):
            @pl.when(sends_to[way])
            def _(way=way):
                for c in halo(r, way):
                    c.start()

    def add_halos(r, out):
        for way in (0, 1):
            plane = 0 if way == 0 else wx - 1

            @pl.when(hears_from[way])
            def _(way=way, plane=plane):
                for m, c in enumerate(halo(r, way)):
                    c.wait_recv()
                for m in range(members):
                    rows = pl.ds((m * wx + plane) * wz, wz)
                    ghost = xghost[r, way, m]
                    if r > 0:
                        ghost = ghost + xextra[way]
                    out[rows, :] += coef[rows, :] * ghost
        for way in (2, 3):
            row = 0 if way == 2 else wz - 1

            @pl.when(hears_from[way])
            def _(way=way, row=row):
                for c in halo(r, way):
                    c.wait_recv()
                for m in range(members):
                    for x in range(wx):
                        at = pl.ds((m * wx + x) * wz + row, 1)
                        ghost = zghost[r, way - 2, m, x : x + 1, :]
                        if r > 0:
                            ghost = ghost + zextra[way - 2, x : x + 1, :]
                        out[at, :] += coef[at, :] * ghost

    def end_sends(r):
        for way in range(4):
            @pl.when(sends_to[way])
            def _(way=way):
                for c in halo(r, way):
                    c.wait_send()

    loads[0].wait()
    pack(now, 0)
    box_peers = jnp.where(box > 0, 1, 0) + jnp.where(box < n_box - 1, 1, 0)
    pl.semaphore_wait(barrier, n_slab - 1 + box_peers)
    send_halos(0)
    for i in (3, 4, 5, 6, 7):
        loads[i].start()

    for i in (1, 2):
        loads[i].wait()
    eye = iota((length, length), 0) == iota((length, length), 1)
    cols = []
    for t in range(steps):
        col = jnp.sum(jnp.where(eye, weights[t : t + 1, :], 0.0), axis=1, keepdims=True)
        cols.append([jnp.where(home[0] == slab * slots + s, col, 0.0) for s in range(slots)])

    def offered(face, t):
        at = pl.ds(pl.multiple_of(face * pts, 128), pts)
        total = cols[t][0] * slabs[pl.ds(0, length), at]
        for s in range(1, slots):
            total = total + cols[t][s] * slabs[pl.ds(s * length, length), at]
        return jnp.sum(total, axis=0, keepdims=True)

    face_x = jnp.where(box == 0, 0, 1)
    face_z = jnp.where(slab == 0, 2, 3)
    common = [offered(f, t) for f in (face_x, 4, 5) for t in range(steps)]
    for kind in range(2):
        vsend[kind] = jnp.concatenate(common + [offered(2 + kind, t) for t in range(steps)], axis=0)

    def give(d):
        peer = lax.rem(slab + d, n_slab)
        return pltpu.make_async_remote_copy(
            vsend.at[jnp.where(peer == 0, 0, 1)], vrecv.at[d - 1], vs_sem.at[d - 1], vr_sem.at[d - 1],
            device_id={"slab": peer}, device_id_type=MESH)

    for d in range(1, n_slab):
        give(d).start()

    for i in (3, 4, 5):
        loads[i].wait()
    bank, total_z = prof.shape
    here = iota((wz, total_z), 1) == slab * wz + iota((wz, total_z), 0)
    for m in reversed(range(members)):
        mine = jnp.sum(jnp.where(iota((bank, total_z), 0) == ids[m], prof[...], 0.0), axis=0, keepdims=True)
        gain = 1.0 + jnp.sum(jnp.where(here, mine, 0.0), axis=1, keepdims=True)
        for x in range(wx):
            coef[pl.ds((m * wx + x) * wz, wz), :] = coef[pl.ds(x * wz, wz), :] * gain

    z_at, y_at = iota((wz, ny), 0), iota((wz, ny), 1)

    def advance(field, before, out):
        def member(m, carry):
            base = m * block
            for x in range(wx):
                rows = pl.ds(pl.multiple_of(base + x * wz, 8), wz)
                c = field[rows, :]
                lap = -6.0 * c
                if x > 0:
                    lap = lap + field[pl.ds(pl.multiple_of(base + (x - 1) * wz, 8), wz), :]
                if x < wx - 1:
                    lap = lap + field[pl.ds(pl.multiple_of(base + (x + 1) * wz, 8), wz), :]
                lap = lap + jnp.where(z_at == 0, 0.0, pltpu.roll(c, 1, 0))
                lap = lap + jnp.where(z_at == wz - 1, 0.0, pltpu.roll(c, wz - 1, 0))
                lap = lap + jnp.where(y_at == 0, 0.0, pltpu.roll(c, 1, 1))
                lap = lap + jnp.where(y_at == ny - 1, 0.0, pltpu.roll(c, ny - 1, 1))
                out[rows, :] = (2.0 * c - before[rows, :]) + coef[rows, :] * lap
            return carry

        lax.fori_loop(0, members, member, 0)

    loads[6].wait()
    advance(now, prev, one)

    loads[7].wait()
    margin, wide = 8, 128

    def where_is(face):
        cell = cells[pl.ds(face, 1), :]
        cx = quotient(cell, total_z * ny)
        rest = cell - cx * (total_z * ny)
        cz = quotient(rest, ny)
        return cx - box * wx, cz - slab * wz, rest - cz * ny

    def hot(cols, col_of):
        return jnp.where(iota((cols, pts), 0) == col_of, 1.0, 0.0).astype(BF16)

    px, pz, py = where_is(face_x)
    px_valid = (px >= 0) & (px < wx)
    px_row = pz + margin
    hot_x[...] = hot(ny, py)
    px, pz, py = where_is(face_z)
    pz_valid = (pz >= 0) & (pz < wz)
    pz_row = px + margin
    hot_z[...] = hot(ny, py)
    px, pz, py = where_is(4)
    low_row = pz + margin
    hot_low[...] = hot(wide, px + margin)
    px, pz, py = where_is(5)
    high_row = pz + margin
    hot_high[...] = hot(wide, px + margin)

    add_halos(0, one)
    pack(one, 1)
    send_halos(1)

    for d in range(1, n_slab):
        give(d).wait_recv()
    values = vsend[jnp.where(slab == 0, 0, 1)]
    for d in range(1, n_slab):
        values = values + vrecv[d - 1]

    def rows_of(k):
        return [values[2 * k + t : 2 * k + t + 1] for t in range(steps)]

    tall_x, tall_z = wx + 2 * margin, wz + 2 * margin
    always = low_row >= -tall_z * n_slab * pts
    on_x = place(tall_z, px_row, px_valid, rows_of(0), hot_x[...])
    on_z = place(tall_x, pz_row, pz_valid, rows_of(3), hot_z[...])
    low_y = place(tall_z, low_row, always, rows_of(1), hot_low[...])
    high_y = place(tall_z, high_row, always, rows_of(2), hot_high[...])
    plane_x = jnp.where(box == 0, 0, wx - 1)
    row_z = jnp.where(slab == 0, 0, wz - 1) + margin
    tall_row, tall_lane = iota((tall_z, ny), 0), iota((tall_z, ny), 1)

    def source_plane(t, x):
        at = x + margin
        out = jnp.where(tall_row == row_z, on_z[t][at : at + 1, :], 0.0)
        out = out + jnp.where(tall_lane == 0, low_y[t][:, at : at + 1], 0.0)
        out = out + jnp.where(tall_lane == ny - 1, high_y[t][:, at : at + 1], 0.0)
        if x in (0, wx - 1):
            out = out + jnp.where(plane_x == x, on_x[t], 0.0)
        return out

    def add_source(t, out):
        for x in range(wx):
            plane = source_plane(t, x)
            if t == 0:
                zextra[0, x : x + 1, :] = plane[margin - 1 : margin]
                zextra[1, x : x + 1, :] = plane[margin + wz : margin + wz + 1]
            for m in range(members):
                out[pl.ds((m * wx + x) * wz, wz), :] += plane[margin : margin + wz]
        if t == 0:
            xextra[0] = source_plane(t, -1)[margin : margin + wz]
            xextra[1] = source_plane(t, wx)[margin : margin + wz]

    add_source(0, one)
    advance(one, now, two)
    add_source(1, two)
    add_halos(1, two)
    end_sends(0)
    end_sends(1)
    for d in range(1, n_slab):
        give(d).wait_send()


def store_kernel(two, one, next_h, last_h, sem):
    copies = [pltpu.make_async_copy(src, dst, sem.at[i]) for i, (src, dst) in enumerate(((two, next_h), (one, last_h)))]
    for c in copies:
        c.start()
    for c in copies:
        c.wait()


def on_device(pressure_now, pressure_prev, courant_sq, member_profiles, member_ids, stored_slabs,
              slab_home, interp_weights, surface_cells):
    members, wx, wz, ny = pressure_now.shape
    slots, length, points = stored_slabs.shape
    pts = surface_cells.shape[1]
    n_box, n_slab = lax.axis_size("box"), lax.axis_size("slab")
    dims = (members, wx, wz, ny, slots, length, pts, n_box, n_slab)
    rows = members * wx * wz
    vmem = pl.BlockSpec(memory_space=pltpu.VMEM)
    in_hbm = lambda a: pltpu.with_memory_space_constraint(a, pltpu.HBM)
    hbm = pl.BlockSpec(memory_space=pltpu.HBM)
    field = jax.ShapeDtypeStruct((rows, ny), F32)
    dma = pltpu.SemaphoreType.DMA
    new, last = pl.pallas_call(
        functools.partial(kernel, dims),
        out_shape=(field, field),
        in_specs=[pl.BlockSpec(memory_space=pltpu.SMEM)] + [hbm] * 8,
        out_specs=(vmem, vmem),
        scratch_shapes=[
            pltpu.SMEM(member_ids.shape, I32),
            pltpu.VMEM(member_profiles.shape, F32), pltpu.VMEM(interp_weights.shape, F32),
            pltpu.VMEM(surface_cells.shape, I32),
            pltpu.VMEM((rows, ny), F32), pltpu.VMEM((rows, ny), F32), pltpu.VMEM((rows, ny), F32),
            pltpu.VMEM((slots * length, points), F32),
            pltpu.VMEM((2, members, wz, ny), F32),
            pltpu.VMEM((2, 2, members, wx, ny), F32),
            pltpu.VMEM((2, 2, members, wz, ny), F32),
            pltpu.VMEM((2, 2, members, wx, ny), F32),
            pltpu.VMEM((2, wz, ny), F32), pltpu.VMEM((2, wx, ny), F32),
            pltpu.VMEM((ny, pts), BF16), pltpu.VMEM((ny, pts), BF16),
            pltpu.VMEM((128, pts), BF16), pltpu.VMEM((128, pts), BF16),
            pltpu.VMEM((2, 8, pts), F32),
            pltpu.VMEM((n_slab - 1, 8, pts), F32),
            dma((8,)), dma((2, 4, members)), dma((2, 4, members)),
            dma((n_slab - 1,)), dma((n_slab - 1,)),
        ],
        compiler_params=pltpu.CompilerParams(collective_id=0, has_side_effects=True,
                                             vmem_limit_bytes=32 * 1024 * 1024),
    )(slab_home, *(in_hbm(a) for a in (
        member_ids, member_profiles, interp_weights, surface_cells,
        pressure_now.reshape(rows, ny), pressure_prev.reshape(rows, ny),
        courant_sq.reshape(wx * wz, ny), stored_slabs.reshape(slots * length, points),
    )))
    placed = pltpu.HBM((rows, ny), F32)
    new, last = pl.pallas_call(
        store_kernel,
        out_shape=(placed, placed),
        in_specs=[vmem, vmem],
        out_specs=(hbm, hbm),
        scratch_shapes=[dma((2,))],
        compiler_params=pltpu.CompilerParams(vmem_limit_bytes=4 * 1024 * 1024),
    )(new, last)
    return new.reshape(pressure_now.shape), last.reshape(pressure_now.shape)


def solution(mesh):
    in_specs = (
        P("ens", "box", "slab", None), P("ens", "box", "slab", None), P("box", "slab", None), P(),
        P("ens"), P("slab", None, None), P("ens"), P(), P(),
    )
    out_specs = (P("ens", "box", "slab", None), P("ens", "box", "slab", None))
    return jax.shard_map(on_device, mesh=mesh, in_specs=in_specs, out_specs=out_specs, check_vma=False)
```
